256 devices in a mesh: grp: 16 (over x, y), dev: 16 (over z, core).
Axes of the slice: x: 4, y: 4, z: 8, core: 2. Of those that a mesh axis runs over, the one named last changes fastest.
Arguments:
- q_lat: bfloat16 [1024, 64, 576], P(('grp', 'dev')), parts along dimension 0, may hold values from -40 to 40
- latent_cache: bfloat16 [1024, 256, 576], P(('grp', 'dev')), parts along dimension 0, may hold values from -8 to 8
- lengths: int32 [1024], P('grp'), parts along dimension 0, may hold values from 32 to 256, as said below
- moves: int32 [512, 3], P('grp'), parts along dimension 0, may hold values from 0 to 63, as said below
- hidden_in: bfloat16 [1024, 3584], P(('grp', 'dev')), parts along dimension 0, may hold values from -6 to 6
- norm_gain: bfloat16 [3584], replicated, may hold values from 0.25 to 1.75
- w_up: bfloat16 [3584, 10240], P(None, 'dev'), may hold values from -0.09375 to 0.09375
- w_down: bfloat16 [10240, 3584], P('dev'), may hold values from -0.0625 to 0.0625
- queue_counts: int32 [256, 8], P(('grp', 'dev')), parts along dimension 0, may hold values from 0 to 63
- deadline: int32 [1024], P(('grp', 'dev')), parts along dimension 0, may hold values from 0 to 7
Outputs:
- attn_out: bfloat16 [1024, 64, 512], P(('grp', 'dev')), parts along dimension 0
- new_cache: bfloat16 [1024, 256, 576], P(('grp', 'dev')), parts along dimension 0
- mixed: bfloat16 [1024, 3584], P(('grp', 'dev')), parts along dimension 0
- bucket_load: float32 [128], P('grp'), parts along dimension 0
The draws below stay inside these ranges and needn't reach their ends.
There are 16 independent parts, one for each index of `grp`. The reference program is written for one: setup_inputs(seed, part) draws one part's arguments, and reference() takes and returns one part's arrays. A program takes and returns all parts, laid end to end along the dimension named above; an argument that names none is the same for every part. Nothing has to cross between parts.
Inputs may be any that keep to these rules, and one draw needn't show every extreme that they name: `lengths`: every length is at least 32; some request has exactly 256. `moves`: entry j * 16 + s (j below 2) has source device s and names a request of device s (requests r lie on device r // 4); the requests listed for one device are distinct. In round j every source s sends to (s + k_j) mod 16, with k_j between 1 and 15 the same for all sources of the round and different between rounds; one of the rounds has k_j = 8.
All inputs are finite; a program needn't handle non-finite values.
Results may differ from the reference program's by a relative error of at most 0.002.
The reference program's roundings to bfloat16 on the way count: a program that leaves them out, or rounds other values in their place, can miss the bound.
Values may be sent and summed in bfloat16 or wider, within the bound.
No kernel may reach another device: no remote copies, remote signals or barrier semaphores. Data moves between devices by JAX's collectives and lax.ppermute only.
A program may use at most 128 MiB of HBM per device.

```python
import jax
import jax.numpy as jnp
from jax import lax

D = 3584
FF = 10240
H = 64
KV = 576
VL = 512
CTX = 256
ROWS_DEV = 4
MOVE_DEV = 2
BUCKETS = 8
ROWS = 64
MOVES = 32
N_DEV = 16


def latent_pair(key):
    base_key = jax.random.fold_in(key, 7)
    key_cache, key_query = jax.random.split(base_key, 2)
    latent = jnp.clip(jax.random.normal(key_cache, (ROWS, CTX, KV), jnp.float32), -6.0, 6.0)
    queries = jnp.clip(jax.random.normal(key_query, (ROWS, H, KV), jnp.float32), -6.0, 6.0)
    return (queries, latent)


def draw_q_lat(key, part):
    return latent_pair(key)[0].astype(jnp.bfloat16)


def draw_latent_cache(key, part):
    return latent_pair(key)[1].astype(jnp.bfloat16)


def draw_lengths(key, part):
    key_level, key_spread, key_pick = jax.random.split(jax.random.fold_in(key, 21), 3)
    groups = ROWS // ROWS_DEV
    level = jax.random.randint(key_level, (groups,), 1, 5)
    ceiling = jnp.repeat(CTX * level // 4, ROWS_DEV)
    lowest = CTX // 8
    spread = jax.random.randint(key_spread, (ROWS,), 0, 1 << 20)
    values = lowest + spread % (ceiling - lowest + 1)
    chosen = jax.random.randint(key_pick, (), 0, ROWS)
    values = jnp.where(jnp.arange(ROWS) == chosen, CTX, values)
    return values.astype(jnp.int32)


def draw_moves(key, part):
    key_offset, key_rows, key_place = jax.random.split(jax.random.fold_in(key, 31), 3)
    groups = ROWS // ROWS_DEV
    half = groups // 2
    others = jax.random.permutation(key_offset, max(groups - 2, 1))[:MOVE_DEV - 1] + 1
    others = others + (others >= half).astype(others.dtype)
    listed = jnp.concatenate([jnp.full((1,), half, others.dtype), others])
    place = jax.random.randint(key_place, (), 0, MOVE_DEV)
    offsets = jnp.roll(listed, place)
    row_keys = jax.random.split(key_rows, groups)
    picked = jax.vmap(lambda single: jax.random.permutation(single, ROWS_DEV)[:MOVE_DEV])(row_keys)
    sources = jnp.arange(groups)
    requests = sources[None, :] * ROWS_DEV + picked.T
    targets = (sources[None, :] + offsets[:, None]) % groups
    senders = jnp.broadcast_to(sources[None, :], (MOVE_DEV, groups))
    return jnp.stack([requests, senders, targets], axis=-1).reshape(MOVES, 3).astype(jnp.int32)


def with_ends(values, own_key, least, high):
    longest = values.shape.index(max(values.shape))
    spots = []
    for shift in (0, 1):
        where = [jax.random.randint(jax.random.fold_in(own_key, axis), (), 0, length) for axis, length in enumerate(values.shape)]
        where[longest] = (where[longest] + shift) % values.shape[longest]
        spots.append(tuple(where))
    return values.at[spots[0]].set(least).at[spots[1]].set(high)


def steps_of(stream_key, extent, pieces, least, top_value):
    level = 1.0
    for axis_at, blocks in pieces:
        draws = jax.random.uniform(jax.random.fold_in(jax.random.fold_in(stream_key, 6), axis_at), (blocks,), jnp.float32, least / len(pieces), top_value / len(pieces))
        level = level * jnp.repeat(jnp.exp(draws), extent[axis_at] // blocks).reshape((-1,) + (1,) * (len(extent) - 1 - axis_at))
    return level


def scatter_about(rng, dims, scale, most, cuts=(), held_as=jnp.bfloat16):
    entries = scale * jax.random.normal(rng, dims, jnp.float32)
    if cuts:
        entries = entries * steps_of(rng, dims, cuts, -0.22, 0.18)
    return jnp.clip(entries, -most, most).astype(held_as)


def setup_inputs(seed: int = 0, part: int = 0) -> dict:
    key_of = jax.random.split(jax.random.key(seed), 11)
    own_keys = jax.random.split(jax.random.fold_in(key_of[10], part), 11)
    return {
        "q_lat": draw_q_lat(jax.random.fold_in(jax.random.fold_in(key_of[10], part), 71), part),
        "latent_cache": draw_latent_cache(jax.random.fold_in(jax.random.fold_in(key_of[10], part), 71), part),
        "lengths": draw_lengths(jax.random.fold_in(jax.random.fold_in(key_of[10], part), 71), part),
        "moves": draw_moves(jax.random.fold_in(jax.random.fold_in(key_of[10], part), 71), part),
        "hidden_in": scatter_about(own_keys[4], (ROWS, D), 1.0, 6.0, ((0, 16),)),
        "norm_gain": jnp.clip(1.0 + 0.15 * jax.random.normal(key_of[5], (D,), jnp.float32), 0.25, 1.75).astype(jnp.bfloat16),
        "w_up": scatter_about(key_of[6], (D, FF), D ** -0.5, 0.09375, ((1, 16),)),
        "w_down": scatter_about(key_of[7], (FF, D), FF ** -0.5, 0.0625, ((0, 16),)),
        "queue_counts": with_ends(jax.random.randint(own_keys[8], (N_DEV, BUCKETS), 0, 64), jax.random.fold_in(own_keys[8], 1), 0, 63).astype(jnp.int32),
        "deadline": with_ends(jax.random.randint(own_keys[9], (ROWS,), 0, BUCKETS), jax.random.fold_in(own_keys[9], 1), 0, BUCKETS - 1).astype(jnp.int32),
    }


softmax_scale = 192.0 ** (-0.5)

def attention(queries, latent, context_lengths):
    query_wide = queries.astype(jnp.float32)
    latent_wide = latent.astype(jnp.float32)
    scores = jnp.einsum('rhc,rkc->rhk', query_wide, latent_wide) * softmax_scale
    included = jnp.arange(CTX, dtype=jnp.int32)[None, None, :] < context_lengths[:, None, None]
    scores = jnp.where(included, scores, jnp.float32(-1e+30))
    largest = lax.optimization_barrier(jnp.max(scores, axis=-1, keepdims=True))
    weights = jnp.where(included, jnp.exp(scores - largest), jnp.float32(0.0))
    total = lax.optimization_barrier(jnp.sum(weights, axis=-1))
    rounded = lax.optimization_barrier(weights.astype(jnp.bfloat16))
    summed = jnp.einsum('rhk,rkc->rhc', rounded.astype(jnp.float32), latent_wide[:, :, :VL])
    return (summed / total[:, :, None]).astype(jnp.bfloat16)

def reference(q_lat, latent_cache, lengths, moves, hidden_in, norm_gain, w_up, w_down, queue_counts, deadline):
    attn_out = attention(q_lat, latent_cache, lengths)
    rounds = moves.reshape(MOVE_DEV, N_DEV, 3)
    source_rows = rounds[:, :, 0]
    target_rows = jnp.take_along_axis(source_rows, rounds[:, :, 2], axis=1)
    new_cache = latent_cache.at[target_rows.reshape(-1)].set(latent_cache[source_rows.reshape(-1)])
    widened = hidden_in.astype(jnp.float32)
    scaled = lax.rsqrt(lax.optimization_barrier(jnp.mean(widened * widened, axis=-1, keepdims=True)) + 1e-06)
    normed = (widened * scaled * norm_gain.astype(jnp.float32)[None, :]).astype(jnp.bfloat16)
    upward = jnp.dot(normed, w_up, preferred_element_type=jnp.float32)
    hidden = jax.nn.silu(upward).astype(jnp.bfloat16)
    downward = jnp.dot(hidden, w_down, preferred_element_type=jnp.float32)
    mixed = (widened + downward).astype(jnp.bfloat16)
    running = (deadline[:, None] == jnp.arange(BUCKETS, dtype=jnp.int32)[None, :]).astype(jnp.float32)
    bucket_load = lax.optimization_barrier(jnp.sum(queue_counts.astype(jnp.float32), axis=0)) + lax.optimization_barrier(jnp.sum(running, axis=0))
    return (attn_out, new_cache, mixed, bucket_load)
```

```python
from functools import partial

import jax
import jax.numpy as jnp
from jax import lax
from jax.experimental import pallas as pl
from jax.experimental.pallas import tpu as pltpu
from jax.sharding import PartitionSpec as P


VL = 512
CONTEXT = 256
BUCKETS = 8
LANES = 128
MIB = 1 << 20

softmax_scale = 192.0 ** (-0.5)

VMEM = pltpu.VMEM
SMEM = pltpu.SMEM
HBM = pltpu.HBM


def whole(space):
    return pl.BlockSpec(memory_space=space)


def shifted(value, axis, steps):
    count = lax.axis_size(axis)
    pairs = [(source, (source + steps) % count) for source in range(count)]
    return lax.ppermute(value, axis, pairs)


def piece_windows(count, depth, lanes):
    across = CONTEXT // lanes
    down = count // across
    return [
        (pl.ds((i % down) * depth, depth), pl.ds((i // down) * lanes, lanes))
        for i in range(count)
    ]


def prepare_kernel(
    devices, moves_ref, cache_ref, hidden_ref, gain_ref, queue_ref, deadline_ref,
    half_ref, pieces_ref, rows_ref, info_ref, sems,
):
    me = lax.axis_index("dev")
    own_rows = cache_ref.shape[0]
    leaving = [moves_ref[0, j * devices + me] - me * own_rows for j in range(2)]
    distance = [
        (moves_ref[2, j * devices + me] - me + devices) % devices for j in range(2)
    ]
    first_is_half = distance[0] == devices // 2
    half_row = jnp.where(first_is_half, leaving[0], leaving[1])
    other_row = jnp.where(first_is_half, leaving[1], leaving[0])
    info_ref[0] = jnp.where(first_is_half, distance[1], distance[0])
    info_ref[1] = half_row
    info_ref[2] = other_row
    copies = [
        pltpu.make_async_copy(cache_ref.at[half_row], half_ref, sems.at[0]),
    ] + [
        pltpu.make_async_copy(
            cache_ref.at[other_row, rows, lanes], pieces_ref.at[i], sems.at[1 + i]
        )
        for i, (rows, lanes) in enumerate(piece_windows(*pieces_ref.shape))
    ]
    for copy in copies:
        copy.start()
    features = hidden_ref.shape[1]
    wide = hidden_ref[...].astype(jnp.float32)
    scaled = lax.rsqrt(jnp.mean(wide * wide, axis=-1, keepdims=True) + 1e-06)
    normed = wide * scaled * gain_ref[...].astype(jnp.float32)[None, :]
    block_rows = 2 * own_rows
    place = lax.broadcasted_iota(jnp.int32, (block_rows, features), 0) // own_rows
    doubled = jnp.concatenate([normed, normed], axis=0)
    rows_ref[:, 0:features] = jnp.where(place == me % 2, doubled, 0.0).astype(jnp.bfloat16)
    extra = rows_ref.shape[1] - features
    lane = lax.broadcasted_iota(jnp.int32, (block_rows, extra), 1)
    row = lax.broadcasted_iota(jnp.int32, (block_rows, extra), 0)
    counts = jnp.zeros((block_rows, extra), jnp.int32)
    for b in range(BUCKETS):
        count = queue_ref[0, b]
        for r in range(own_rows):
            count = count + (deadline_ref[r] == b).astype(jnp.int32)
        counts = jnp.where(lane == b, count, counts)
    counts = jnp.where(row == (me % 2) * own_rows, counts, 0)
    rows_ref[:, features:] = counts.astype(jnp.float32).astype(jnp.bfloat16)
    for copy in copies:
        copy.wait()


def prepare(moves, cache, hidden_in, norm_gain, queue_counts, deadline):
    devices = lax.axis_size("dev")
    own_rows, depth, context = cache.shape
    features = hidden_in.shape[1]
    return pl.pallas_call(
        partial(prepare_kernel, devices),
        out_shape=(
            jax.ShapeDtypeStruct((depth, context), cache.dtype),
            jax.ShapeDtypeStruct(
                (devices, depth * context // (devices * LANES), LANES), cache.dtype
            ),
            jax.ShapeDtypeStruct((2 * own_rows, features + 2 * LANES), jnp.bfloat16),
            jax.ShapeDtypeStruct((3,), jnp.int32),
        ),
        in_specs=[
            whole(SMEM), whole(HBM), whole(VMEM), whole(VMEM), whole(SMEM), whole(SMEM),
        ],
        out_specs=(whole(VMEM), whole(VMEM), whole(VMEM), whole(SMEM)),
        scratch_shapes=[pltpu.SemaphoreType.DMA((devices + 1,))],
        name="prepare",
    )(moves, cache, hidden_in, norm_gain, queue_counts, deadline)


def attend_kernel(lengths_ref, queries_ref, cache_ref, out_ref, kept_ref):
    own_rows = pl.num_programs(0)
    row = pl.program_id(0)
    length = lengths_ref[lax.axis_index("dev") * own_rows + row]
    latent = cache_ref[0]
    kept_ref[0] = latent
    scores = (
        jnp.dot(queries_ref[0], latent, preferred_element_type=jnp.float32) * softmax_scale
    )
    included = lax.broadcasted_iota(jnp.int32, scores.shape, 1) < length
    scores = jnp.where(included, scores, jnp.float32(-1e30))
    largest = jnp.max(scores, axis=-1, keepdims=True)
    weights = jnp.where(included, jnp.exp(scores - largest), jnp.float32(0.0))
    total = jnp.sum(weights, axis=-1, keepdims=True)
    summed = lax.dot_general(
        weights.astype(jnp.bfloat16),
        latent[0:VL, :],
        (((1,), (1,)), ((), ())),
        preferred_element_type=jnp.float32,
    )
    out_ref[0] = (summed / total).astype(jnp.bfloat16)


def attend(lengths, queries, cache):
    own_rows, heads, depth = queries.shape
    context = cache.shape[2]
    block = lambda *dims: pl.BlockSpec((1, *dims), lambda r: (r, 0, 0))
    return pl.pallas_call(
        attend_kernel,
        grid=(own_rows,),
        out_shape=(
            jax.ShapeDtypeStruct((own_rows, heads, VL), jnp.bfloat16),
            jax.ShapeDtypeStruct(cache.shape, cache.dtype),
        ),
        in_specs=[whole(SMEM), block(heads, depth), block(depth, context)],
        out_specs=(block(heads, VL), block(depth, context)),
        compiler_params=pltpu.CompilerParams(vmem_limit_bytes=12 * MIB),
        name="attend",
    )(lengths, queries, cache)


def feed_kernel(
    own_ref, near_ref, next_ref, far_ref, other_near_ref, other_next_ref, other_far_ref,
    up_ref, down_ref,
    own_out, give_out, keep_out, give_far_out, keep_far_out, load_ref,
    rows_buf, up_buf, down_buf, up_sems, down_sems,
):
    pieces, depth, _ = up_buf.shape
    columns = down_buf.shape[2]
    up_copies = [
        pltpu.make_async_copy(
            up_ref.at[pl.ds(i * depth, depth), :], up_buf.at[i], up_sems.at[i]
        )
        for i in range(pieces)
    ]
    down_copies = [
        pltpu.make_async_copy(
            down_ref.at[:, pl.ds(i * columns, columns)], down_buf.at[i], down_sems.at[i]
        )
        for i in range(down_buf.shape[0])
    ]
    for copy in up_copies + down_copies:
        copy.start()
    first_core = lax.axis_index("dev") % 2 == 0
    block = own_ref.shape[0]
    width = own_ref.shape[1]
    for at, part in (
        (0, own_ref), (1, near_ref), (2, next_ref), (4, other_near_ref), (5, other_next_ref),
    ):
        rows_buf[at * block : at * block + part.shape[0], :] = part[...]
    far = far_ref[...]
    other_far = other_far_ref[...]
    rows_buf[7 * block :, 0 : width // 2] = jnp.where(first_core, far, other_far)
    rows_buf[7 * block :, width // 2 :] = jnp.where(first_core, other_far, far)
    features = pieces * depth
    counts = rows_buf[:, features : features + LANES].astype(jnp.float32)
    load_ref[...] = jnp.sum(counts, axis=0)[0:BUCKETS]
    up = None
    for i in range(pieces):
        up_copies[i].wait()
        term = jnp.dot(
            rows_buf[:, i * depth : (i + 1) * depth],
            up_buf[i],
            preferred_element_type=jnp.float32,
        )
        up = term if up is None else up + term
    hidden = (up / (1.0 + jnp.exp(-up))).astype(jnp.bfloat16)
    half = features // 2
    for i, copy in enumerate(down_copies):
        copy.wait()
        product = jnp.dot(hidden, down_buf[i], preferred_element_type=jnp.float32)
        at = slice(i * columns, (i + 1) * columns)
        own_out[:, at] = product[0:block]
        give_out[:, at] = product[block : 4 * block]
        keep_out[:, at] = product[4 * block : 7 * block]
        far_sums = product[7 * block :]
        for low, high in ((0, half), (half, features)):
            start, stop = max(low, i * columns), min(high, (i + 1) * columns)
            if start < stop:
                piece = far_sums[:, start - i * columns : stop - i * columns]
                target = slice(start - low, stop - low)
                mine = first_core if low == 0 else jnp.logical_not(first_core)

                @pl.when(mine)
                def _(piece=piece, target=target):
                    keep_far_out[:, target] = piece

                @pl.when(jnp.logical_not(mine))
                def _(piece=piece, target=target):
                    give_far_out[:, target] = piece


def feed(parts, w_up, w_down):
    features, units = w_up.shape
    pieces = 7
    depth = features // pieces
    block, width = parts[0].shape
    wide = lambda rows, columns: jax.ShapeDtypeStruct((rows, columns), jnp.float32)
    return pl.pallas_call(
        feed_kernel,
        out_shape=(
            wide(block, features),
            wide(3 * block, features),
            wide(3 * block, features),
            wide(block, features // 2),
            wide(block, features // 2),
            jax.ShapeDtypeStruct((BUCKETS,), jnp.float32),
        ),
        in_specs=[whole(VMEM)] * 7 + [whole(HBM)] * 2,
        out_specs=(whole(VMEM),) * 6,
        scratch_shapes=[
            pltpu.VMEM((8 * block, width), jnp.bfloat16),
            pltpu.VMEM((pieces, depth, units), w_up.dtype),
            pltpu.VMEM((pieces, units, depth), w_down.dtype),
            pltpu.SemaphoreType.DMA((pieces,)),
            pltpu.SemaphoreType.DMA((pieces,)),
        ],
        compiler_params=pltpu.CompilerParams(vmem_limit_bytes=20 * MIB),
        name="feed",
    )(*parts, w_up, w_down)


def turn_kernel(devices, info_ref, pieces_ref, out_ref):
    steps = info_ref[0]
    for d in range(devices):
        out_ref[d] = pieces_ref[(d - steps + devices) % devices]


def turn(info, pieces):
    return pl.pallas_call(
        partial(turn_kernel, pieces.shape[0]),
        out_shape=jax.ShapeDtypeStruct(pieces.shape, pieces.dtype),
        in_specs=[whole(SMEM), whole(VMEM)],
        out_specs=whole(VMEM),
        compiler_params=pltpu.CompilerParams(vmem_limit_bytes=4 * MIB),
        name="turn",
    )(info, pieces)


def patch_half_kernel(info_ref, half_ref, kept_ref, out_ref, sem):
    copy = pltpu.make_async_copy(half_ref, out_ref.at[info_ref[1]], sem)
    copy.start()
    copy.wait()


def patch_half(info, half, kept):
    return pl.pallas_call(
        patch_half_kernel,
        out_shape=jax.ShapeDtypeStruct(kept.shape, kept.dtype),
        in_specs=[whole(SMEM), whole(VMEM), whole(pl.ANY)],
        out_specs=whole(pl.ANY),
        input_output_aliases={2: 0},
        scratch_shapes=[pltpu.SemaphoreType.DMA],
        compiler_params=pltpu.CompilerParams(vmem_limit_bytes=4 * MIB),
        name="patch_half",
    )(info, half, kept)


def patch_pieces_kernel(info_ref, pieces_ref, kept_ref, out_ref, sems):
    copies = [
        pltpu.make_async_copy(
            pieces_ref.at[i], out_ref.at[info_ref[2], rows, lanes], sems.at[i]
        )
        for i, (rows, lanes) in enumerate(piece_windows(*pieces_ref.shape))
    ]
    for copy in copies:
        copy.start()
    for copy in copies:
        copy.wait()


def patch_pieces(info, pieces, kept):
    return pl.pallas_call(
        patch_pieces_kernel,
        out_shape=jax.ShapeDtypeStruct(kept.shape, kept.dtype),
        in_specs=[whole(SMEM), whole(VMEM), whole(pl.ANY)],
        out_specs=whole(pl.ANY),
        input_output_aliases={2: 0},
        scratch_shapes=[pltpu.SemaphoreType.DMA((pieces.shape[0],))],
        compiler_params=pltpu.CompilerParams(vmem_limit_bytes=4 * MIB),
        name="patch_pieces",
    )(info, pieces, kept)


def exchange(value):
    return lax.all_to_all(value, "dev", 0, 0, tiled=True)


def swapped(value):
    count = lax.axis_size("dev")
    return lax.ppermute(value, "dev", [(s, s ^ 1) for s in range(count)])


def outward(value, chips):
    count = lax.axis_size("dev")
    pairs = [(s, (s + (2 * chips if s % 2 == 0 else -2 * chips)) % count) for s in range(count)]
    return lax.ppermute(value, "dev", pairs)


SHRINK = 0.25


def narrow(x):
    return (x * SHRINK).astype(jnp.float16)


def widen(x):
    return x.astype(jnp.float32) * (1.0 / SHRINK)


def per_device(
    q_lat, latent_cache, lengths, moves, hidden_in, norm_gain, w_up, w_down, queue_counts, deadline
):
    devices = lax.axis_size("dev")
    own_rows, _ = hidden_in.shape
    first_core = lax.axis_index("dev") % 2 == 0
    block = 2 * own_rows
    cache = jnp.swapaxes(latent_cache, 1, 2)
    half, pieces, rows, info = prepare(
        moves.T, cache, hidden_in, norm_gain, queue_counts, deadline
    )
    own = rows + swapped(rows)
    width = own.shape[1] // 2
    far = outward(jnp.where(first_core, own[:, :width], own[:, width:]), 4)
    near = outward(own, 1)
    pieces = exchange(pieces)
    nxt = outward(jnp.concatenate([own, near], axis=0), 2)
    half = shifted(half, "dev", devices // 2)
    attn_out, kept = attend(lengths, q_lat, cache)
    other_near = swapped(near)
    other_far = swapped(far)
    other_next = swapped(nxt)
    own_sums, give, keep, give_far, keep_far, load = feed(
        (own, near, nxt, far, other_near, other_next, other_far), w_up, w_down
    )
    pieces = turn(info, pieces)
    got_far = swapped(give_far)
    got = swapped(give)
    sums_far = outward(narrow(keep_far + got_far), 4)
    sums_next = outward(narrow(keep[block:] + got[block:]), 2)
    pieces = exchange(pieces)
    kept = patch_half(info, half, kept)
    near_sums = keep[:block] + got[:block] + widen(sums_next[block:])
    sums_near = outward(narrow(near_sums), 1)
    wide_far = widen(sums_far)
    zeros = jnp.zeros_like(wide_far)
    both = jnp.concatenate(
        [jnp.where(first_core, wide_far, zeros), jnp.where(first_core, zeros, wide_far)],
        axis=1,
    )
    total = own_sums + widen(sums_next[:block]) + widen(sums_near) + both
    low, high = total[:own_rows], total[own_rows:]
    got_total = swapped(jnp.where(first_core, high, low))
    summed = jnp.where(first_core, low, high) + got_total
    mixed = (hidden_in.astype(jnp.float32) + summed).astype(jnp.bfloat16)
    kept = patch_pieces(info, pieces, kept)
    return attn_out, jnp.swapaxes(kept, 1, 2), mixed, load


def solution(mesh):
    return jax.shard_map(
        per_device,
        mesh=mesh,
        in_specs=(
            P(("grp", "dev"), None, None),
            P(("grp", "dev"), None, None),
            P("grp"),
            P("grp", None),
            P(("grp", "dev"), None),
            P(),
            P(None, "dev"),
            P("dev", None),
            P(("grp", "dev"), None),
            P(("grp", "dev")),
        ),
        out_specs=(
            P(("grp", "dev"), None, None),
            P(("grp", "dev"), None, None),
            P(("grp", "dev"), None),
            P("grp"),
        ),
        check_vma=False,
    )
```

```python
from functools import partial

import jax
import jax.numpy as jnp
from jax import lax
from jax.experimental import pallas as pl
from jax.experimental.pallas import tpu as pltpu
from jax.sharding import PartitionSpec as P


VL = 512
CONTEXT = 256
BUCKETS = 8
LANES = 128
MIB = 1 << 20

softmax_scale = 192.0 ** (-0.5)

VMEM = pltpu.VMEM
SMEM = pltpu.SMEM
HBM = pltpu.HBM


def in_hbm(x):
    return pltpu.with_memory_space_constraint(x, HBM)


def in_vmem(x):
    return pltpu.with_memory_space_constraint(x, VMEM)


def whole(space):
    return pl.BlockSpec(memory_space=space)


def shifted(value, axis, steps):
    count = lax.axis_size(axis)
    pairs = [(source, (source + steps) % count) for source in range(count)]
    return lax.ppermute(value, axis, pairs)


def piece_windows(count, depth, lanes):
    across = CONTEXT // lanes
    down = count // across
    return [
        (pl.ds((i % down) * depth, depth), pl.ds((i // down) * lanes, lanes))
        for i in range(count)
    ]


def rows_kernel(hidden_ref, gain_ref, queue_ref, deadline_ref, rows_ref):
    me = lax.axis_index("dev")
    own_rows, features = hidden_ref.shape
    wide = hidden_ref[...].astype(jnp.float32)
    scaled = lax.rsqrt(jnp.mean(wide * wide, axis=-1, keepdims=True) + 1e-06)
    normed = wide * scaled * gain_ref[...].astype(jnp.float32)[None, :]
    block_rows = 2 * own_rows
    place = lax.broadcasted_iota(jnp.int32, (block_rows, features), 0) // own_rows
    doubled = jnp.concatenate([normed, normed], axis=0)
    rows_ref[:, 0:features] = jnp.where(place == me % 2, doubled, 0.0).astype(jnp.bfloat16)
    extra = rows_ref.shape[1] - features
    lane = lax.broadcasted_iota(jnp.int32, (block_rows, extra), 1)
    row = lax.broadcasted_iota(jnp.int32, (block_rows, extra), 0)
    counts = jnp.zeros((block_rows, extra), jnp.int32)
    for b in range(BUCKETS):
        count = queue_ref[0, b]
        for r in range(own_rows):
            count = count + (deadline_ref[r] == b).astype(jnp.int32)
        counts = jnp.where(lane == b, count, counts)
    counts = jnp.where(row == (me % 2) * own_rows, counts, 0)
    rows_ref[:, features:] = counts.astype(jnp.float32).astype(jnp.bfloat16)


def make_rows(hidden_in, norm_gain, queue_counts, deadline):
    own_rows, features = hidden_in.shape
    return pl.pallas_call(
        rows_kernel,
        out_shape=pltpu.VMEM((2 * own_rows, features + 2 * LANES), jnp.bfloat16),
        in_specs=[whole(VMEM), whole(VMEM), whole(SMEM), whole(SMEM)],
        out_specs=whole(VMEM),
        name="rows",
    )(hidden_in, norm_gain, queue_counts, deadline)


def payload_kernel(devices, moves_ref, cache_ref, half_ref, pieces_ref, info_ref, sems):
    me = lax.axis_index("dev")
    own_rows = cache_ref.shape[0]
    leaving = [moves_ref[0, j * devices + me] - me * own_rows for j in range(2)]
    distance = [
        (moves_ref[2, j * devices + me] - me + devices) % devices for j in range(2)
    ]
    first_is_half = distance[0] == devices // 2
    half_row = jnp.where(first_is_half, leaving[0], leaving[1])
    other_row = jnp.where(first_is_half, leaving[1], leaving[0])
    info_ref[0] = jnp.where(first_is_half, distance[1], distance[0])
    info_ref[1] = half_row
    info_ref[2] = other_row
    copies = [
        pltpu.make_async_copy(
            cache_ref.at[other_row, rows, lanes], pieces_ref.at[i], sems.at[1 + i]
        )
        for i, (rows, lanes) in enumerate(piece_windows(*pieces_ref.shape))
    ]
    copies.append(pltpu.make_async_copy(cache_ref.at[half_row], half_ref, sems.at[0]))
    for copy in copies:
        copy.start()
    for copy in copies:
        copy.wait()


def make_payload(moves, cache):
    devices = lax.axis_size("dev")
    _, depth, context = cache.shape
    return pl.pallas_call(
        partial(payload_kernel, devices),
        out_shape=(
            pltpu.VMEM((depth, context), cache.dtype),
            pltpu.VMEM((devices, depth * context // (devices * LANES), LANES), cache.dtype),
            jax.ShapeDtypeStruct((3,), jnp.int32),
        ),
        in_specs=[whole(SMEM), whole(HBM)],
        out_specs=(whole(VMEM), whole(VMEM), whole(SMEM)),
        scratch_shapes=[pltpu.SemaphoreType.DMA((devices + 1,))],
        name="payload",
    )(moves, in_hbm(cache))


def attention(queries, latent, length):
    scores = jnp.dot(queries, latent, preferred_element_type=jnp.float32) * softmax_scale
    included = lax.broadcasted_iota(jnp.int32, scores.shape, 1) < length
    scores = jnp.where(included, scores, jnp.float32(-1e30))
    largest = jnp.max(scores, axis=-1, keepdims=True)
    weights = jnp.where(included, jnp.exp(scores - largest), jnp.float32(0.0))
    total = jnp.sum(weights, axis=-1, keepdims=True)
    summed = lax.dot_general(
        weights.astype(jnp.bfloat16),
        latent[0:VL, :],
        (((1,), (1,)), ((), ())),
        preferred_element_type=jnp.float32,
    )
    return (summed / total).astype(jnp.bfloat16)


def attend_kernel(
    lengths_ref, queries_ref, cache_ref, up_ref, down_ref,
    attn_ref, kept_ref, up_out, down_out,
    queries_buf, cache_buf, attn_buf, lengths_buf,
    in_sems, kept_sems, attn_sems, weight_sems, lengths_sem,
):
    own_rows = queries_buf.shape[0]
    me = lax.axis_index("dev")
    lengths_copy = pltpu.make_async_copy(lengths_ref, lengths_buf, lengths_sem)
    lengths_copy.start()
    in_copies = [
        (
            pltpu.make_async_copy(cache_ref.at[r], cache_buf.at[r], in_sems.at[2 * r]),
            pltpu.make_async_copy(queries_ref.at[r], queries_buf.at[r], in_sems.at[2 * r + 1]),
        )
        for r in range(own_rows)
    ]
    out_copies = [
        pltpu.make_async_copy(up_ref, up_out, weight_sems.at[0]),
        pltpu.make_async_copy(down_ref, down_out, weight_sems.at[1]),
    ]
    for pair in in_copies:
        for copy in pair:
            copy.start()
    for copy in out_copies:
        copy.start()
    lengths_copy.wait()
    for r in range(own_rows):
        for copy in in_copies[r]:
            copy.wait()
        kept = pltpu.make_async_copy(cache_buf.at[r], kept_ref.at[r], kept_sems.at[r])
        kept.start()
        attn_buf[r] = attention(
            queries_buf[r], cache_buf[r], lengths_buf[me * own_rows + r]
        )
        done = pltpu.make_async_copy(attn_buf.at[r], attn_ref.at[r], attn_sems.at[r])
        done.start()
        out_copies += [kept, done]
    for copy in out_copies:
        copy.wait()


def attend(lengths, queries, cache, w_up, w_down):
    own_rows, heads, _ = queries.shape
    return pl.pallas_call(
        attend_kernel,
        out_shape=(
            jax.ShapeDtypeStruct((own_rows, heads, VL), jnp.bfloat16),
            jax.ShapeDtypeStruct(cache.shape, cache.dtype),
            pltpu.VMEM(w_up.shape, w_up.dtype),
            pltpu.VMEM(w_down.shape, w_down.dtype),
        ),
        in_specs=[whole(HBM)] * 5,
        out_specs=(whole(HBM),) * 2 + (whole(VMEM),) * 2,
        scratch_shapes=[
            pltpu.VMEM(queries.shape, queries.dtype),
            pltpu.VMEM(cache.shape, cache.dtype),
            pltpu.VMEM((own_rows, heads, VL), jnp.bfloat16),
            pltpu.SMEM(lengths.shape, jnp.int32),
            pltpu.SemaphoreType.DMA((2 * own_rows,)),
            pltpu.SemaphoreType.DMA((own_rows,)),
            pltpu.SemaphoreType.DMA((own_rows,)),
            pltpu.SemaphoreType.DMA((2,)),
            pltpu.SemaphoreType.DMA,
        ],
        compiler_params=pltpu.CompilerParams(vmem_limit_bytes=12 * MIB),
        name="attend",
    )(in_hbm(lengths), in_hbm(queries), in_hbm(cache), in_hbm(w_up), in_hbm(w_down))


def feed_kernel(
    up_ref, down_ref,
    own_ref, near_ref, next_ref, far_ref, other_near_ref, other_next_ref, other_far_ref,
    own_out, give_out, keep_out, give_far_out, keep_far_out, load_ref,
    rows_buf,
):
    features, _ = up_ref.shape
    columns = features // 7
    first_core = lax.axis_index("dev") % 2 == 0
    block = own_ref.shape[0]
    width = own_ref.shape[1]
    for at, part in (
        (0, own_ref), (1, near_ref), (2, next_ref), (4, other_near_ref), (5, other_next_ref),
    ):
        rows_buf[at * block : at * block + part.shape[0], :] = part[...]
    far = far_ref[...]
    other_far = other_far_ref[...]
    rows_buf[7 * block :, 0 : width // 2] = jnp.where(first_core, far, other_far)
    rows_buf[7 * block :, width // 2 :] = jnp.where(first_core, other_far, far)
    counts = rows_buf[:, features : features + LANES].astype(jnp.float32)
    load_ref[...] = jnp.sum(counts, axis=0)[0:BUCKETS]
    up = jnp.dot(rows_buf[:, 0:features], up_ref[...], preferred_element_type=jnp.float32)
    hidden = (up / (1.0 + jnp.exp(-up))).astype(jnp.bfloat16)
    half = features // 2
    for i in range(features // columns):
        at = slice(i * columns, (i + 1) * columns)
        product = jnp.dot(hidden, down_ref[:, at], preferred_element_type=jnp.float32)
        own_out[:, at] = product[0:block]
        give_out[:, at] = product[block : 4 * block]
        keep_out[:, at] = product[4 * block : 7 * block]
        far_sums = product[7 * block :]
        for low, high in ((0, half), (half, features)):
            start, stop = max(low, i * columns), min(high, (i + 1) * columns)
            if start < stop:
                piece = far_sums[:, start - i * columns : stop - i * columns]
                target = slice(start - low, stop - low)
                mine = first_core if low == 0 else jnp.logical_not(first_core)

                @pl.when(mine)
                def _(piece=piece, target=target):
                    keep_far_out[:, target] = piece

                @pl.when(jnp.logical_not(mine))
                def _(piece=piece, target=target):
                    give_far_out[:, target] = piece


def feed(w_up, w_down, parts):
    features, _ = w_up.shape
    block, row_width = parts[0].shape
    wide = lambda rows, columns: pltpu.VMEM((rows, columns), jnp.float32)
    return pl.pallas_call(
        feed_kernel,
        out_shape=(
            wide(block, features),
            wide(3 * block, features),
            wide(3 * block, features),
            wide(block, features // 2),
            wide(block, features // 2),
            jax.ShapeDtypeStruct((BUCKETS,), jnp.float32),
        ),
        in_specs=[whole(VMEM)] * 9,
        out_specs=(whole(VMEM),) * 6,
        scratch_shapes=[pltpu.VMEM((8 * block, row_width), jnp.bfloat16)],
        compiler_params=pltpu.CompilerParams(vmem_limit_bytes=12 * MIB),
        name="feed",
    )(in_vmem(w_up), in_vmem(w_down), *parts)


def turn_kernel(devices, info_ref, pieces_ref, out_ref, sems):
    steps = info_ref[0]
    copies = [
        pltpu.make_async_copy(
            pieces_ref.at[(d - steps + devices) % devices], out_ref.at[d], sems.at[d]
        )
        for d in range(devices)
    ]
    for copy in copies:
        copy.start()
    for copy in copies:
        copy.wait()


def turn(info, pieces):
    return pl.pallas_call(
        partial(turn_kernel, pieces.shape[0]),
        out_shape=jax.ShapeDtypeStruct(pieces.shape, pieces.dtype),
        in_specs=[whole(SMEM), whole(VMEM)],
        out_specs=whole(HBM),
        scratch_shapes=[pltpu.SemaphoreType.DMA((pieces.shape[0],))],
        compiler_params=pltpu.CompilerParams(vmem_limit_bytes=4 * MIB),
        name="turn",
    )(info, in_vmem(pieces))


def patch_half_kernel(info_ref, half_ref, kept_ref, out_ref, sem):
    copy = pltpu.make_async_copy(half_ref, out_ref.at[info_ref[1]], sem)
    copy.start()
    copy.wait()


def patch_half(info, half, kept):
    return pl.pallas_call(
        patch_half_kernel,
        out_shape=jax.ShapeDtypeStruct(kept.shape, kept.dtype),
        in_specs=[whole(SMEM), whole(VMEM), whole(pl.ANY)],
        out_specs=whole(pl.ANY),
        input_output_aliases={2: 0},
        scratch_shapes=[pltpu.SemaphoreType.DMA],
        compiler_params=pltpu.CompilerParams(vmem_limit_bytes=4 * MIB),
        name="patch_half",
    )(info, half, kept)


def patch_pieces_kernel(info_ref, pieces_ref, kept_ref, out_ref, sems):
    copies = [
        pltpu.make_async_copy(
            pieces_ref.at[i], out_ref.at[info_ref[2], rows, lanes], sems.at[i]
        )
        for i, (rows, lanes) in enumerate(piece_windows(*pieces_ref.shape))
    ]
    for copy in copies:
        copy.start()
    for copy in copies:
        copy.wait()


def patch_pieces(info, pieces, kept):
    return pl.pallas_call(
        patch_pieces_kernel,
        out_shape=jax.ShapeDtypeStruct(kept.shape, kept.dtype),
        in_specs=[whole(SMEM), whole(VMEM), whole(pl.ANY)],
        out_specs=whole(pl.ANY),
        input_output_aliases={2: 0},
        scratch_shapes=[pltpu.SemaphoreType.DMA((pieces.shape[0],))],
        compiler_params=pltpu.CompilerParams(vmem_limit_bytes=4 * MIB),
        name="patch_pieces",
    )(info, pieces, kept)


def exchange(value):
    return lax.all_to_all(value, "dev", 0, 0, tiled=True)


def swapped(value):
    count = lax.axis_size("dev")
    return lax.ppermute(value, "dev", [(s, s ^ 1) for s in range(count)])


def outward(value, chips):
    count = lax.axis_size("dev")
    pairs = [(s, (s + (2 * chips if s % 2 == 0 else -2 * chips)) % count) for s in range(count)]
    return lax.ppermute(value, "dev", pairs)


SHRINK = 0.25


def narrow(x):
    return (x * SHRINK).astype(jnp.float16)


def widen(x):
    return x.astype(jnp.float32) * (1.0 / SHRINK)


def per_device(
    q_lat, latent_cache, lengths, moves, hidden_in, norm_gain, w_up, w_down, queue_counts, deadline
):
    devices = lax.axis_size("dev")
    own_rows, _ = hidden_in.shape
    first_core = lax.axis_index("dev") % 2 == 0
    block = 2 * own_rows
    cache = jnp.swapaxes(latent_cache, 1, 2)
    rows = make_rows(hidden_in, norm_gain, queue_counts, deadline)
    own = rows + swapped(rows)
    half, pieces, info = make_payload(moves.T, cache)
    width = own.shape[1] // 2
    far = outward(jnp.where(first_core, own[:, :width], own[:, width:]), 4)
    near = outward(own, 1)
    pieces = exchange(pieces)
    nxt = outward(jnp.concatenate([own, near], axis=0), 2)
    half = shifted(half, "dev", devices // 2)
    other_near = swapped(near)
    other_far = swapped(far)
    other_next = swapped(nxt)
    attn_out, kept, w_up, w_down = attend(lengths, q_lat, cache, w_up, w_down)
    own_sums, give, keep, give_far, keep_far, load = feed(
        w_up, w_down, (own, near, nxt, far, other_near, other_next, other_far)
    )
    pieces = turn(info, pieces)
    got_far = swapped(give_far)
    got = swapped(give)
    sums_far = outward(narrow(keep_far + got_far), 4)
    sums_next = outward(narrow(keep[block:] + got[block:]), 2)
    pieces = exchange(pieces)
    kept = patch_half(info, half, kept)
    near_sums = keep[:block] + got[:block] + widen(sums_next[block:])
    sums_near = outward(narrow(near_sums), 1)
    wide_far = widen(sums_far)
    zeros = jnp.zeros_like(wide_far)
    both = jnp.concatenate(
        [jnp.where(first_core, wide_far, zeros), jnp.where(first_core, zeros, wide_far)],
        axis=1,
    )
    total = own_sums + widen(sums_next[:block]) + widen(sums_near) + both
    low, high = total[:own_rows], total[own_rows:]
    got_total = swapped(jnp.where(first_core, high, low))
    summed = jnp.where(first_core, low, high) + got_total
    mixed = (hidden_in.astype(jnp.float32) + summed).astype(jnp.bfloat16)
    kept = patch_pieces(info, pieces, kept)
    return attn_out, jnp.swapaxes(kept, 1, 2), mixed, load


def solution(mesh):
    return jax.shard_map(
        per_device,
        mesh=mesh,
        in_specs=(
            P(("grp", "dev"), None, None),
            P(("grp", "dev"), None, None),
            P("grp"),
            P("grp", None),
            P(("grp", "dev"), None),
            P(),
            P(None, "dev"),
            P("dev", None),
            P(("grp", "dev"), None),
            P(("grp", "dev")),
        ),
        out_specs=(
            P(("grp", "dev"), None, None),
            P(("grp", "dev"), None, None),
            P(("grp", "dev"), None),
            P("grp"),
        ),
        check_vma=False,
    )
```

```python
from functools import partial

import jax
import jax.numpy as jnp
from jax import lax
from jax.experimental import pallas as pl
from jax.experimental.pallas import tpu as pltpu
from jax.sharding import PartitionSpec as P


VL = 512
CONTEXT = 256
BUCKETS = 8
LANES = 128
MIB = 1 << 20
AHEAD = 7

softmax_scale = 192.0 ** (-0.5)

VMEM = pltpu.VMEM
SMEM = pltpu.SMEM
HBM = pltpu.HBM


def in_hbm(x):
    return pltpu.with_memory_space_constraint(x, HBM)


def in_vmem(x):
    return pltpu.with_memory_space_constraint(x, VMEM)


def whole(space):
    return pl.BlockSpec(memory_space=space)


def shifted(value, axis, steps):
    count = lax.axis_size(axis)
    pairs = [(source, (source + steps) % count) for source in range(count)]
    return lax.ppermute(value, axis, pairs)


def piece_windows(count, depth, lanes):
    across = CONTEXT // lanes
    down = count // across
    return [
        (pl.ds((i % down) * depth, depth), pl.ds((i // down) * lanes, lanes))
        for i in range(count)
    ]


def rows_kernel(hidden_ref, gain_ref, queue_ref, deadline_ref, rows_ref):
    me = lax.axis_index("dev")
    own_rows, features = hidden_ref.shape
    wide = hidden_ref[...].astype(jnp.float32)
    scaled = lax.rsqrt(jnp.mean(wide * wide, axis=-1, keepdims=True) + 1e-06)
    normed = wide * scaled * gain_ref[...].astype(jnp.float32)[None, :]
    block_rows = 2 * own_rows
    place = lax.broadcasted_iota(jnp.int32, (block_rows, features), 0) // own_rows
    doubled = jnp.concatenate([normed, normed], axis=0)
    rows_ref[:, 0:features] = jnp.where(place == me % 2, doubled, 0.0).astype(jnp.bfloat16)
    extra = rows_ref.shape[1] - features
    lane = lax.broadcasted_iota(jnp.int32, (block_rows, extra), 1)
    row = lax.broadcasted_iota(jnp.int32, (block_rows, extra), 0)
    counts = jnp.zeros((block_rows, extra), jnp.int32)
    for b in range(BUCKETS):
        count = queue_ref[0, b]
        for r in range(own_rows):
            count = count + (deadline_ref[r] == b).astype(jnp.int32)
        counts = jnp.where(lane == b, count, counts)
    counts = jnp.where(row == (me % 2) * own_rows, counts, 0)
    rows_ref[:, features:] = counts.astype(jnp.float32).astype(jnp.bfloat16)


def make_rows(hidden_in, norm_gain, queue_counts, deadline):
    own_rows, features = hidden_in.shape
    return pl.pallas_call(
        rows_kernel,
        out_shape=pltpu.VMEM((2 * own_rows, features + 2 * LANES), jnp.bfloat16),
        in_specs=[whole(VMEM), whole(VMEM), whole(SMEM), whole(SMEM)],
        out_specs=whole(VMEM),
        name="rows",
    )(hidden_in, norm_gain, queue_counts, deadline)


def payload_kernel(devices, moves_ref, cache_ref, half_ref, pieces_ref, info_ref, sems):
    me = lax.axis_index("dev")
    own_rows = cache_ref.shape[0]
    leaving = [moves_ref[0, j * devices + me] - me * own_rows for j in range(2)]
    distance = [
        (moves_ref[2, j * devices + me] - me + devices) % devices for j in range(2)
    ]
    first_is_half = distance[0] == devices // 2
    half_row = jnp.where(first_is_half, leaving[0], leaving[1])
    other_row = jnp.where(first_is_half, leaving[1], leaving[0])
    info_ref[0] = jnp.where(first_is_half, distance[1], distance[0])
    info_ref[1] = half_row
    info_ref[2] = other_row
    copies = [
        pltpu.make_async_copy(
            cache_ref.at[other_row, rows, lanes], pieces_ref.at[i], sems.at[1 + i]
        )
        for i, (rows, lanes) in enumerate(piece_windows(*pieces_ref.shape))
    ]
    copies.append(pltpu.make_async_copy(cache_ref.at[half_row], half_ref, sems.at[0]))
    for copy in copies:
        copy.start()
    for copy in copies:
        copy.wait()


def make_payload(moves, cache):
    devices = lax.axis_size("dev")
    _, depth, context = cache.shape
    return pl.pallas_call(
        partial(payload_kernel, devices),
        out_shape=(
            pltpu.VMEM((depth, context), cache.dtype),
            pltpu.VMEM((devices, depth * context // (devices * LANES), LANES), cache.dtype),
            jax.ShapeDtypeStruct((3,), jnp.int32),
        ),
        in_specs=[whole(SMEM), whole(HBM)],
        out_specs=(whole(VMEM), whole(VMEM), whole(SMEM)),
        scratch_shapes=[pltpu.SemaphoreType.DMA((devices + 1,))],
        name="payload",
    )(moves, in_hbm(cache))


def attention(queries, latent, length):
    scores = jnp.dot(queries, latent, preferred_element_type=jnp.float32) * softmax_scale
    included = lax.broadcasted_iota(jnp.int32, scores.shape, 1) < length
    scores = jnp.where(included, scores, jnp.float32(-1e30))
    largest = jnp.max(scores, axis=-1, keepdims=True)
    weights = jnp.where(included, jnp.exp(scores - largest), jnp.float32(0.0))
    total = jnp.sum(weights, axis=-1, keepdims=True)
    summed = lax.dot_general(
        weights.astype(jnp.bfloat16),
        latent[0:VL, :],
        (((1,), (1,)), ((), ())),
        preferred_element_type=jnp.float32,
    )
    return (summed / total).astype(jnp.bfloat16)


def attend_kernel(
    lengths_ref, queries_ref, cache_ref,
    attn_ref, kept_ref,
    queries_buf, cache_buf, attn_buf, lengths_buf,
    in_sems, kept_sems, attn_sems, lengths_sem,
):
    own_rows = queries_buf.shape[0]
    me = lax.axis_index("dev")
    lengths_copy = pltpu.make_async_copy(lengths_ref, lengths_buf, lengths_sem)
    lengths_copy.start()
    in_copies = [
        (
            pltpu.make_async_copy(cache_ref.at[r], cache_buf.at[r], in_sems.at[2 * r]),
            pltpu.make_async_copy(queries_ref.at[r], queries_buf.at[r], in_sems.at[2 * r + 1]),
        )
        for r in range(own_rows)
    ]
    out_copies = []
    for pair in in_copies:
        for copy in pair:
            copy.start()
    lengths_copy.wait()
    for r in range(own_rows):
        for copy in in_copies[r]:
            copy.wait()
        kept = pltpu.make_async_copy(cache_buf.at[r], kept_ref.at[r], kept_sems.at[r])
        kept.start()
        attn_buf[r] = attention(
            queries_buf[r], cache_buf[r], lengths_buf[me * own_rows + r]
        )
        done = pltpu.make_async_copy(attn_buf.at[r], attn_ref.at[r], attn_sems.at[r])
        done.start()
        out_copies += [kept, done]
    for copy in out_copies:
        copy.wait()


def attend(lengths, queries, cache):
    own_rows, heads, _ = queries.shape
    return pl.pallas_call(
        attend_kernel,
        out_shape=(
            jax.ShapeDtypeStruct((own_rows, heads, VL), jnp.bfloat16),
            jax.ShapeDtypeStruct(cache.shape, cache.dtype),
        ),
        in_specs=[whole(HBM)] * 3,
        out_specs=(whole(HBM),) * 2,
        scratch_shapes=[
            pltpu.VMEM(queries.shape, queries.dtype),
            pltpu.VMEM(cache.shape, cache.dtype),
            pltpu.VMEM((own_rows, heads, VL), jnp.bfloat16),
            pltpu.SMEM(lengths.shape, jnp.int32),
            pltpu.SemaphoreType.DMA((2 * own_rows,)),
            pltpu.SemaphoreType.DMA((own_rows,)),
            pltpu.SemaphoreType.DMA((own_rows,)),
            pltpu.SemaphoreType.DMA,
        ],
        compiler_params=pltpu.CompilerParams(vmem_limit_bytes=12 * MIB),
        name="attend",
    )(in_hbm(lengths), in_hbm(queries), in_hbm(cache))


def feed_kernel(
    up_ref, down_ref,
    own_ref, near_ref, next_ref, far_ref, other_near_ref, other_next_ref, other_far_ref,
    own_out, give_out, keep_out, give_far_out, keep_far_out, load_ref,
    rows_buf, up_buf, down_buf, sems,
):
    pieces, depth, _ = up_buf.shape
    columns = down_buf.shape[2]
    features = pieces * depth
    copies = [
        pltpu.make_async_copy(up_ref.at[pl.ds(i * depth, depth), :], up_buf.at[i], sems.at[i])
        for i in range(pieces)
    ] + [
        pltpu.make_async_copy(
            down_ref.at[:, pl.ds(i * columns, columns)], down_buf.at[i], sems.at[pieces + i]
        )
        for i in range(pieces)
    ]
    for copy in copies[:AHEAD]:
        copy.start()

    def arrive(i):
        copies[i].wait()
        if i + AHEAD < len(copies):
            copies[i + AHEAD].start()

    first_core = lax.axis_index("dev") % 2 == 0
    block = own_ref.shape[0]
    width = own_ref.shape[1]
    for at, part in (
        (0, own_ref), (1, near_ref), (2, next_ref), (4, other_near_ref), (5, other_next_ref),
    ):
        rows_buf[at * block : at * block + part.shape[0], :] = part[...]
    far = far_ref[...]
    other_far = other_far_ref[...]
    rows_buf[7 * block :, 0 : width // 2] = jnp.where(first_core, far, other_far)
    rows_buf[7 * block :, width // 2 :] = jnp.where(first_core, other_far, far)
    counts = rows_buf[:, features : features + LANES].astype(jnp.float32)
    load_ref[...] = jnp.sum(counts, axis=0)[0:BUCKETS]
    up = None
    for i in range(pieces):
        arrive(i)
        term = jnp.dot(
            rows_buf[:, i * depth : (i + 1) * depth],
            up_buf[i],
            preferred_element_type=jnp.float32,
        )
        up = term if up is None else up + term
    hidden = (up / (1.0 + jnp.exp(-up))).astype(jnp.bfloat16)
    half = features // 2
    for i in range(pieces):
        arrive(pieces + i)
        at = slice(i * columns, (i + 1) * columns)
        product = jnp.dot(hidden, down_buf[i], preferred_element_type=jnp.float32)
        own_out[:, at] = product[0:block]
        give_out[:, at] = product[block : 4 * block]
        keep_out[:, at] = product[4 * block : 7 * block]
        far_sums = product[7 * block :]
        for low, high in ((0, half), (half, features)):
            start, stop = max(low, i * columns), min(high, (i + 1) * columns)
            if start < stop:
                piece = far_sums[:, start - i * columns : stop - i * columns]
                target = slice(start - low, stop - low)
                mine = first_core if low == 0 else jnp.logical_not(first_core)

                @pl.when(mine)
                def _(piece=piece, target=target):
                    keep_far_out[:, target] = piece

                @pl.when(jnp.logical_not(mine))
                def _(piece=piece, target=target):
                    give_far_out[:, target] = piece


def feed(w_up, w_down, parts):
    features, units = w_up.shape
    pieces = 7
    block, row_width = parts[0].shape
    wide = lambda rows, columns: pltpu.VMEM((rows, columns), jnp.float32)
    return pl.pallas_call(
        feed_kernel,
        out_shape=(
            wide(block, features),
            wide(3 * block, features),
            wide(3 * block, features),
            wide(block, features // 2),
            wide(block, features // 2),
            jax.ShapeDtypeStruct((BUCKETS,), jnp.float32),
        ),
        in_specs=[whole(HBM)] * 2 + [whole(VMEM)] * 7,
        out_specs=(whole(VMEM),) * 6,
        scratch_shapes=[
            pltpu.VMEM((8 * block, row_width), jnp.bfloat16),
            pltpu.VMEM((pieces, features // pieces, units), w_up.dtype),
            pltpu.VMEM((pieces, units, features // pieces), w_down.dtype),
            pltpu.SemaphoreType.DMA((2 * pieces,)),
        ],
        compiler_params=pltpu.CompilerParams(vmem_limit_bytes=20 * MIB),
        name="feed",
    )(in_hbm(w_up), in_hbm(w_down), *parts)


def turn_kernel(devices, info_ref, pieces_ref, out_ref, sems):
    steps = info_ref[0]
    copies = [
        pltpu.make_async_copy(
            pieces_ref.at[(d - steps + devices) % devices], out_ref.at[d], sems.at[d]
        )
        for d in range(devices)
    ]
    for copy in copies:
        copy.start()
    for copy in copies:
        copy.wait()


def turn(info, pieces):
    return pl.pallas_call(
        partial(turn_kernel, pieces.shape[0]),
        out_shape=jax.ShapeDtypeStruct(pieces.shape, pieces.dtype),
        in_specs=[whole(SMEM), whole(VMEM)],
        out_specs=whole(HBM),
        scratch_shapes=[pltpu.SemaphoreType.DMA((pieces.shape[0],))],
        compiler_params=pltpu.CompilerParams(vmem_limit_bytes=4 * MIB),
        name="turn",
    )(info, in_vmem(pieces))


def patch_half_kernel(info_ref, half_ref, kept_ref, out_ref, sem):
    copy = pltpu.make_async_copy(half_ref, out_ref.at[info_ref[1]], sem)
    copy.start()
    copy.wait()


def patch_half(info, half, kept):
    return pl.pallas_call(
        patch_half_kernel,
        out_shape=jax.ShapeDtypeStruct(kept.shape, kept.dtype),
        in_specs=[whole(SMEM), whole(VMEM), whole(pl.ANY)],
        out_specs=whole(pl.ANY),
        input_output_aliases={2: 0},
        scratch_shapes=[pltpu.SemaphoreType.DMA],
        compiler_params=pltpu.CompilerParams(vmem_limit_bytes=4 * MIB),
        name="patch_half",
    )(info, half, kept)


def patch_pieces_kernel(info_ref, pieces_ref, kept_ref, out_ref, sems):
    copies = [
        pltpu.make_async_copy(
            pieces_ref.at[i], out_ref.at[info_ref[2], rows, lanes], sems.at[i]
        )
        for i, (rows, lanes) in enumerate(piece_windows(*pieces_ref.shape))
    ]
    for copy in copies:
        copy.start()
    for copy in copies:
        copy.wait()


def patch_pieces(info, pieces, kept):
    return pl.pallas_call(
        patch_pieces_kernel,
        out_shape=jax.ShapeDtypeStruct(kept.shape, kept.dtype),
        in_specs=[whole(SMEM), whole(VMEM), whole(pl.ANY)],
        out_specs=whole(pl.ANY),
        input_output_aliases={2: 0},
        scratch_shapes=[pltpu.SemaphoreType.DMA((pieces.shape[0],))],
        compiler_params=pltpu.CompilerParams(vmem_limit_bytes=4 * MIB),
        name="patch_pieces",
    )(info, pieces, kept)


def exchange(value):
    return lax.all_to_all(value, "dev", 0, 0, tiled=True)


def swapped(value):
    count = lax.axis_size("dev")
    return lax.ppermute(value, "dev", [(s, s ^ 1) for s in range(count)])


def outward(value, chips):
    count = lax.axis_size("dev")
    pairs = [(s, (s + (2 * chips if s % 2 == 0 else -2 * chips)) % count) for s in range(count)]
    return lax.ppermute(value, "dev", pairs)


SHRINK = 0.25


def narrow(x):
    return (x * SHRINK).astype(jnp.float16)


def widen(x):
    return x.astype(jnp.float32) * (1.0 / SHRINK)


def per_device(
    q_lat, latent_cache, lengths, moves, hidden_in, norm_gain, w_up, w_down, queue_counts, deadline
):
    devices = lax.axis_size("dev")
    own_rows, _ = hidden_in.shape
    first_core = lax.axis_index("dev") % 2 == 0
    block = 2 * own_rows
    cache = jnp.swapaxes(latent_cache, 1, 2)
    rows = make_rows(hidden_in, norm_gain, queue_counts, deadline)
    own = rows + swapped(rows)
    half, pieces, info = make_payload(moves.T, cache)
    width = own.shape[1] // 2
    far = outward(jnp.where(first_core, own[:, :width], own[:, width:]), 4)
    near = outward(own, 1)
    pieces = exchange(pieces)
    nxt = outward(jnp.concatenate([own, near], axis=0), 2)
    half = shifted(half, "dev", devices // 2)
    other_near = swapped(near)
    other_far = swapped(far)
    other_next = swapped(nxt)
    attn_out, kept = attend(lengths, q_lat, cache)
    own_sums, give, keep, give_far, keep_far, load = feed(
        w_up, w_down, (own, near, nxt, far, other_near, other_next, other_far)
    )
    pieces = turn(info, pieces)
    got_far = swapped(give_far)
    got = swapped(give)
    sums_far = outward(narrow(keep_far + got_far), 4)
    pair_sums = keep + got
    near_sums = jnp.concatenate([pair_sums[:block], pair_sums[2 * block :]], axis=0)
    sums_near = outward(narrow(near_sums), 1)
    pieces = exchange(pieces)
    kept = patch_half(info, half, kept)
    next_sums = pair_sums[block : 2 * block] + widen(sums_near[block:])
    sums_next = outward(narrow(next_sums), 2)
    wide_far = widen(sums_far)
    zeros = jnp.zeros_like(wide_far)
    both = jnp.concatenate(
        [jnp.where(first_core, wide_far, zeros), jnp.where(first_core, zeros, wide_far)],
        axis=1,
    )
    total = own_sums + widen(sums_near[:block]) + widen(sums_next) + both
    low, high = total[:own_rows], total[own_rows:]
    got_total = swapped(jnp.where(first_core, high, low))
    summed = jnp.where(first_core, low, high) + got_total
    mixed = (hidden_in.astype(jnp.float32) + summed).astype(jnp.bfloat16)
    kept = patch_pieces(info, pieces, kept)
    return attn_out, jnp.swapaxes(kept, 1, 2), mixed, load


def solution(mesh):
    return jax.shard_map(
        per_device,
        mesh=mesh,
        in_specs=(
            P(("grp", "dev"), None, None),
            P(("grp", "dev"), None, None),
            P("grp"),
            P("grp", None),
            P(("grp", "dev"), None),
            P(),
            P(None, "dev"),
            P("dev", None),
            P(("grp", "dev"), None),
            P(("grp", "dev")),
        ),
        out_specs=(
            P(("grp", "dev"), None, None),
            P(("grp", "dev"), None, None),
            P(("grp", "dev"), None),
            P("grp"),
        ),
        check_vma=False,
    )
```

```python
from functools import partial

import jax
import jax.numpy as jnp
from jax import lax
from jax.experimental import pallas as pl
from jax.experimental.pallas import tpu as pltpu
from jax.sharding import PartitionSpec as P


VL = 512
CONTEXT = 256
BUCKETS = 8
LANES = 128
MIB = 1 << 20
AHEAD = 7

softmax_scale = 192.0 ** (-0.5)

VMEM = pltpu.VMEM
SMEM = pltpu.SMEM
HBM = pltpu.HBM


def in_hbm(x):
    return pltpu.with_memory_space_constraint(x, HBM)


def in_vmem(x):
    return pltpu.with_memory_space_constraint(x, VMEM)


def whole(space):
    return pl.BlockSpec(memory_space=space)


def shifted(value, axis, steps):
    count = lax.axis_size(axis)
    pairs = [(source, (source + steps) % count) for source in range(count)]
    return lax.ppermute(value, axis, pairs)


def piece_windows(count, depth, lanes):
    across = CONTEXT // lanes
    down = count // across
    return [
        (pl.ds((i % down) * depth, depth), pl.ds((i // down) * lanes, lanes))
        for i in range(count)
    ]


def rows_kernel(hidden_ref, gain_ref, queue_ref, deadline_ref, rows_ref):
    me = lax.axis_index("dev")
    own_rows, features = hidden_ref.shape
    wide = hidden_ref[...].astype(jnp.float32)
    scaled = lax.rsqrt(jnp.mean(wide * wide, axis=-1, keepdims=True) + 1e-06)
    normed = wide * scaled * gain_ref[...].astype(jnp.float32)[None, :]
    block_rows = 2 * own_rows
    place = lax.broadcasted_iota(jnp.int32, (block_rows, features), 0) // own_rows
    doubled = jnp.concatenate([normed, normed], axis=0)
    rows_ref[:, 0:features] = jnp.where(place == me % 2, doubled, 0.0).astype(jnp.bfloat16)
    extra = rows_ref.shape[1] - features
    lane = lax.broadcasted_iota(jnp.int32, (block_rows, extra), 1)
    row = lax.broadcasted_iota(jnp.int32, (block_rows, extra), 0)
    counts = jnp.zeros((block_rows, extra), jnp.int32)
    for b in range(BUCKETS):
        count = queue_ref[0, b]
        for r in range(own_rows):
            count = count + (deadline_ref[r] == b).astype(jnp.int32)
        counts = jnp.where(lane == b, count, counts)
    counts = jnp.where(row == (me % 2) * own_rows, counts, 0)
    rows_ref[:, features:] = counts.astype(jnp.float32).astype(jnp.bfloat16)


def make_rows(hidden_in, norm_gain, queue_counts, deadline):
    own_rows, features = hidden_in.shape
    return pl.pallas_call(
        rows_kernel,
        out_shape=pltpu.VMEM((2 * own_rows, features + 2 * LANES), jnp.bfloat16),
        in_specs=[whole(VMEM), whole(VMEM), whole(SMEM), whole(SMEM)],
        out_specs=whole(VMEM),
        name="rows",
    )(hidden_in, norm_gain, queue_counts, deadline)


def payload_kernel(devices, moves_ref, cache_ref, half_ref, pieces_ref, info_ref, sems):
    me = lax.axis_index("dev")
    own_rows = cache_ref.shape[0]
    leaving = [moves_ref[0, j * devices + me] - me * own_rows for j in range(2)]
    distance = [
        (moves_ref[2, j * devices + me] - me + devices) % devices for j in range(2)
    ]
    first_is_half = distance[0] == devices // 2
    half_row = jnp.where(first_is_half, leaving[0], leaving[1])
    other_row = jnp.where(first_is_half, leaving[1], leaving[0])
    info_ref[0] = jnp.where(first_is_half, distance[1], distance[0])
    info_ref[1] = half_row
    info_ref[2] = other_row
    copies = [
        pltpu.make_async_copy(
            cache_ref.at[other_row, rows, lanes], pieces_ref.at[i], sems.at[1 + i]
        )
        for i, (rows, lanes) in enumerate(piece_windows(*pieces_ref.shape))
    ]
    copies.append(pltpu.make_async_copy(cache_ref.at[half_row], half_ref, sems.at[0]))
    for copy in copies:
        copy.start()
    for copy in copies:
        copy.wait()


def make_payload(moves, cache):
    devices = lax.axis_size("dev")
    _, depth, context = cache.shape
    return pl.pallas_call(
        partial(payload_kernel, devices),
        out_shape=(
            pltpu.VMEM((depth, context), cache.dtype),
            pltpu.VMEM((devices, depth * context // (devices * LANES), LANES), cache.dtype),
            jax.ShapeDtypeStruct((3,), jnp.int32),
        ),
        in_specs=[whole(SMEM), whole(HBM)],
        out_specs=(whole(VMEM), whole(VMEM), whole(SMEM)),
        scratch_shapes=[pltpu.SemaphoreType.DMA((devices + 1,))],
        name="payload",
    )(moves, in_hbm(cache))


def attention(queries, latent, length):
    scores = jnp.dot(queries, latent, preferred_element_type=jnp.float32) * softmax_scale
    included = lax.broadcasted_iota(jnp.int32, scores.shape, 1) < length
    scores = jnp.where(included, scores, jnp.float32(-1e30))
    largest = jnp.max(scores, axis=-1, keepdims=True)
    weights = jnp.where(included, jnp.exp(scores - largest), jnp.float32(0.0))
    total = jnp.sum(weights, axis=-1, keepdims=True)
    summed = lax.dot_general(
        weights.astype(jnp.bfloat16),
        latent[0:VL, :],
        (((1,), (1,)), ((), ())),
        preferred_element_type=jnp.float32,
    )
    return (summed / total).astype(jnp.bfloat16)


def attend_kernel(
    lengths_ref, queries_ref, cache_ref,
    attn_ref, kept_ref,
    queries_buf, cache_buf, attn_buf, lengths_buf,
    in_sems, kept_sems, attn_sems, lengths_sem,
):
    own_rows = queries_buf.shape[0]
    me = lax.axis_index("dev")
    lengths_copy = pltpu.make_async_copy(lengths_ref, lengths_buf, lengths_sem)
    lengths_copy.start()
    in_copies = [
        (
            pltpu.make_async_copy(cache_ref.at[r], cache_buf.at[r], in_sems.at[2 * r]),
            pltpu.make_async_copy(queries_ref.at[r], queries_buf.at[r], in_sems.at[2 * r + 1]),
        )
        for r in range(own_rows)
    ]
    out_copies = []
    for pair in in_copies:
        for copy in pair:
            copy.start()
    lengths_copy.wait()
    for r in range(own_rows):
        for copy in in_copies[r]:
            copy.wait()
        kept = pltpu.make_async_copy(cache_buf.at[r], kept_ref.at[r], kept_sems.at[r])
        kept.start()
        attn_buf[r] = attention(
            queries_buf[r], cache_buf[r], lengths_buf[me * own_rows + r]
        )
        done = pltpu.make_async_copy(attn_buf.at[r], attn_ref.at[r], attn_sems.at[r])
        done.start()
        out_copies += [kept, done]
    for copy in out_copies:
        copy.wait()


def attend(lengths, queries, cache):
    own_rows, heads, _ = queries.shape
    return pl.pallas_call(
        attend_kernel,
        out_shape=(
            jax.ShapeDtypeStruct((own_rows, heads, VL), jnp.bfloat16),
            jax.ShapeDtypeStruct(cache.shape, cache.dtype),
        ),
        in_specs=[whole(HBM)] * 3,
        out_specs=(whole(HBM),) * 2,
        scratch_shapes=[
            pltpu.VMEM(queries.shape, queries.dtype),
            pltpu.VMEM(cache.shape, cache.dtype),
            pltpu.VMEM((own_rows, heads, VL), jnp.bfloat16),
            pltpu.SMEM(lengths.shape, jnp.int32),
            pltpu.SemaphoreType.DMA((2 * own_rows,)),
            pltpu.SemaphoreType.DMA((own_rows,)),
            pltpu.SemaphoreType.DMA((own_rows,)),
            pltpu.SemaphoreType.DMA,
        ],
        compiler_params=pltpu.CompilerParams(vmem_limit_bytes=12 * MIB),
        name="attend",
    )(in_hbm(lengths), in_hbm(queries), in_hbm(cache))


def feed_kernel(
    up_ref, down_ref,
    own_ref, near_ref, next_ref, far_ref, other_ref, other_far_ref,
    own_out, give_out, keep_out, keep_far_out, load_ref,
    rows_buf, up_buf, down_buf, sems,
):
    pieces, depth, _ = up_buf.shape
    columns = down_buf.shape[2]
    features = pieces * depth
    copies = [
        pltpu.make_async_copy(up_ref.at[pl.ds(i * depth, depth), :], up_buf.at[i], sems.at[i])
        for i in range(pieces)
    ] + [
        pltpu.make_async_copy(
            down_ref.at[:, pl.ds(i * columns, columns)], down_buf.at[i], sems.at[pieces + i]
        )
        for i in range(pieces)
    ]
    for copy in copies[:AHEAD]:
        copy.start()

    def arrive(i):
        copies[i].wait()
        if i + AHEAD < len(copies):
            copies[i + AHEAD].start()

    first_core = lax.axis_index("dev") % 2 == 0
    block = own_ref.shape[0]
    width = own_ref.shape[1]
    for at, part in (
        (0, own_ref), (1, near_ref), (2, next_ref), (4, other_ref),
    ):
        rows_buf[at * block : at * block + part.shape[0], :] = part[...]
    far = far_ref[...]
    other_far = other_far_ref[...]
    rows_buf[7 * block :, 0 : width // 2] = jnp.where(first_core, far, other_far)
    rows_buf[7 * block :, width // 2 :] = jnp.where(first_core, other_far, far)
    counts = rows_buf[:, features : features + LANES].astype(jnp.float32)
    load_ref[...] = jnp.sum(counts, axis=0)[0:BUCKETS]
    up = None
    for i in range(pieces):
        arrive(i)
        term = jnp.dot(
            rows_buf[:, i * depth : (i + 1) * depth],
            up_buf[i],
            preferred_element_type=jnp.float32,
        )
        up = term if up is None else up + term
    hidden = (up / (1.0 + jnp.exp(-up))).astype(jnp.bfloat16)
    half = features // 2
    for i in range(pieces):
        arrive(pieces + i)
        at = slice(i * columns, (i + 1) * columns)
        product = jnp.dot(hidden, down_buf[i], preferred_element_type=jnp.float32)
        own_out[:, at] = product[0:block]
        give_out[0 : 3 * block, at] = product[block : 4 * block]
        keep_out[:, at] = product[4 * block : 7 * block]
        far_sums = product[7 * block :]
        for low, high in ((0, half), (half, features)):
            start, stop = max(low, i * columns), min(high, (i + 1) * columns)
            if start < stop:
                piece = far_sums[:, start - i * columns : stop - i * columns]
                target = slice(start - low, stop - low)
                mine = first_core if low == 0 else jnp.logical_not(first_core)

                @pl.when(mine)
                def _(piece=piece, target=target):
                    keep_far_out[:, target] = piece

                @pl.when(jnp.logical_not(mine))
                def _(piece=piece, target=target):
                    give_out[3 * block :, target] = piece


def feed(w_up, w_down, parts):
    features, units = w_up.shape
    pieces = 7
    block, row_width = parts[0].shape
    wide = lambda rows, columns: pltpu.VMEM((rows, columns), jnp.float32)
    return pl.pallas_call(
        feed_kernel,
        out_shape=(
            wide(block, features),
            wide(4 * block, features),
            wide(3 * block, features),
            wide(block, features // 2),
            jax.ShapeDtypeStruct((BUCKETS,), jnp.float32),
        ),
        in_specs=[whole(HBM)] * 2 + [whole(VMEM)] * 6,
        out_specs=(whole(VMEM),) * 5,
        scratch_shapes=[
            pltpu.VMEM((8 * block, row_width), jnp.bfloat16),
            pltpu.VMEM((pieces, features // pieces, units), w_up.dtype),
            pltpu.VMEM((pieces, units, features // pieces), w_down.dtype),
            pltpu.SemaphoreType.DMA((2 * pieces,)),
        ],
        compiler_params=pltpu.CompilerParams(vmem_limit_bytes=20 * MIB),
        name="feed",
    )(in_hbm(w_up), in_hbm(w_down), *parts)


def turn_kernel(devices, info_ref, pieces_ref, out_ref, sems):
    steps = info_ref[0]
    copies = [
        pltpu.make_async_copy(
            pieces_ref.at[(d - steps + devices) % devices], out_ref.at[d], sems.at[d]
        )
        for d in range(devices)
    ]
    for copy in copies:
        copy.start()
    for copy in copies:
        copy.wait()


def turn(info, pieces):
    return pl.pallas_call(
        partial(turn_kernel, pieces.shape[0]),
        out_shape=jax.ShapeDtypeStruct(pieces.shape, pieces.dtype),
        in_specs=[whole(SMEM), whole(VMEM)],
        out_specs=whole(HBM),
        scratch_shapes=[pltpu.SemaphoreType.DMA((pieces.shape[0],))],
        compiler_params=pltpu.CompilerParams(vmem_limit_bytes=4 * MIB),
        name="turn",
    )(info, in_vmem(pieces))


def patch_half_kernel(info_ref, half_ref, kept_ref, out_ref, sem):
    copy = pltpu.make_async_copy(half_ref, out_ref.at[info_ref[1]], sem)
    copy.start()
    copy.wait()


def patch_half(info, half, kept):
    return pl.pallas_call(
        patch_half_kernel,
        out_shape=jax.ShapeDtypeStruct(kept.shape, kept.dtype),
        in_specs=[whole(SMEM), whole(VMEM), whole(pl.ANY)],
        out_specs=whole(pl.ANY),
        input_output_aliases={2: 0},
        scratch_shapes=[pltpu.SemaphoreType.DMA],
        compiler_params=pltpu.CompilerParams(vmem_limit_bytes=4 * MIB),
        name="patch_half",
    )(info, half, kept)


def patch_pieces_kernel(info_ref, pieces_ref, kept_ref, out_ref, sems):
    copies = [
        pltpu.make_async_copy(
            pieces_ref.at[i], out_ref.at[info_ref[2], rows, lanes], sems.at[i]
        )
        for i, (rows, lanes) in enumerate(piece_windows(*pieces_ref.shape))
    ]
    for copy in copies:
        copy.start()
    for copy in copies:
        copy.wait()


def patch_pieces(info, pieces, kept):
    return pl.pallas_call(
        patch_pieces_kernel,
        out_shape=jax.ShapeDtypeStruct(kept.shape, kept.dtype),
        in_specs=[whole(SMEM), whole(VMEM), whole(pl.ANY)],
        out_specs=whole(pl.ANY),
        input_output_aliases={2: 0},
        scratch_shapes=[pltpu.SemaphoreType.DMA((pieces.shape[0],))],
        compiler_params=pltpu.CompilerParams(vmem_limit_bytes=4 * MIB),
        name="patch_pieces",
    )(info, pieces, kept)


def exchange(value):
    return lax.all_to_all(value, "dev", 0, 0, tiled=True)


def swapped(value):
    count = lax.axis_size("dev")
    return lax.ppermute(value, "dev", [(s, s ^ 1) for s in range(count)])


def outward(value, chips):
    count = lax.axis_size("dev")
    pairs = [(s, (s + (2 * chips if s % 2 == 0 else -2 * chips)) % count) for s in range(count)]
    return lax.ppermute(value, "dev", pairs)


SHRINK = 0.25


def narrow(x):
    return (x * SHRINK).astype(jnp.float16)


def widen(x):
    return x.astype(jnp.float32) * (1.0 / SHRINK)


def per_device(
    q_lat, latent_cache, lengths, moves, hidden_in, norm_gain, w_up, w_down, queue_counts, deadline
):
    devices = lax.axis_size("dev")
    own_rows, features = hidden_in.shape
    first_core = lax.axis_index("dev") % 2 == 0
    block = 2 * own_rows
    cache = jnp.swapaxes(latent_cache, 1, 2)
    rows = make_rows(hidden_in, norm_gain, queue_counts, deadline)
    own = rows + swapped(rows)
    half, pieces, info = make_payload(moves.T, cache)
    width = own.shape[1] // 2
    far = outward(jnp.where(first_core, own[:, :width], own[:, width:]), 4)
    near = outward(own, 1)
    pieces = exchange(pieces)
    nxt = outward(jnp.concatenate([own, near], axis=0), 2)
    half = shifted(half, "dev", devices // 2)
    other_far = swapped(far)
    other = swapped(jnp.concatenate([near, nxt], axis=0))
    attn_out, kept = attend(lengths, q_lat, cache)
    own_sums, give, keep, keep_far, load = feed(
        w_up, w_down, (own, near, nxt, far, other, other_far)
    )
    pieces = turn(info, pieces)
    got = swapped(give)
    got, got_far = got[: 3 * block], got[3 * block :, : features // 2]
    sums_far = outward(narrow(keep_far + got_far), 4)
    pair_sums = keep + got
    near_sums = jnp.concatenate([pair_sums[:block], pair_sums[2 * block :]], axis=0)
    sums_near = outward(narrow(near_sums), 1)
    pieces = exchange(pieces)
    kept = patch_half(info, half, kept)
    next_sums = pair_sums[block : 2 * block] + widen(sums_near[block:])
    sums_next = outward(narrow(next_sums), 2)
    wide_far = widen(sums_far)
    zeros = jnp.zeros_like(wide_far)
    both = jnp.concatenate(
        [jnp.where(first_core, wide_far, zeros), jnp.where(first_core, zeros, wide_far)],
        axis=1,
    )
    total = own_sums + widen(sums_near[:block]) + widen(sums_next) + both
    low, high = total[:own_rows], total[own_rows:]
    got_total = swapped(jnp.where(first_core, high, low))
    summed = jnp.where(first_core, low, high) + got_total
    mixed = (hidden_in.astype(jnp.float32) + summed).astype(jnp.bfloat16)
    kept = patch_pieces(info, pieces, kept)
    return attn_out, jnp.swapaxes(kept, 1, 2), mixed, load


def solution(mesh):
    return jax.shard_map(
        per_device,
        mesh=mesh,
        in_specs=(
            P(("grp", "dev"), None, None),
            P(("grp", "dev"), None, None),
            P("grp"),
            P("grp", None),
            P(("grp", "dev"), None),
            P(),
            P(None, "dev"),
            P("dev", None),
            P(("grp", "dev"), None),
            P(("grp", "dev")),
        ),
        out_specs=(
            P(("grp", "dev"), None, None),
            P(("grp", "dev"), None, None),
            P(("grp", "dev"), None),
            P("grp"),
        ),
        check_vma=False,
    )
```
